32 devices in a mesh: row: 8 (over z, core), col: 4 (over y, x).
Axes of the slice: x: 2, y: 2, z: 4, core: 2. Of those that a mesh axis runs over, the one named last changes fastest.
Arguments:
- x_fwd: bfloat16 [512, 6144], P('row', 'col'), may hold values from -6 to 6
- x_bwd: bfloat16 [512, 6144], P('row', 'col'), may hold values from -6 to 6
- grad_out: bfloat16 [512, 6144], P('row', 'col'), may hold values from -1.5 to 1.5
- gain: float32 [6144], P('col'), may hold values from 0.1 to 1.9
- w_up: bfloat16 [6144, 12288], P('col', 'row'), may hold values from -0.078125 to 0.078125
- w_down: bfloat16 [12288, 6144], P('row', 'col'), may hold values from -0.0546875 to 0.0546875
Outputs:
- y_fwd: bfloat16 [512, 6144], P('row', 'col')
- dx_bwd: bfloat16 [512, 6144], P('row', 'col')
- step_up: float32 [6144, 12288], P('col', 'row')
- step_down: float32 [12288, 6144], P('row', 'col')
- step_gain: float32 [6144], P('col')
- grad_rms: float32 [], replicated
The draws below stay inside these ranges and needn't reach their ends.
All inputs are finite; a program needn't handle non-finite values.
Results may differ from the reference program's by a relative error of at most 0.0017.
The reference program's roundings to bfloat16 on the way count: a program that leaves them out, or rounds other values in their place, can miss the bound.
Values may be sent and summed in bfloat16 or wider, within the bound.
A program may use at most 128 MiB of HBM per device.

```python
import math
import jax
import jax.numpy as jnp
from jax import lax

D = 6144
FF = 12288
TOKENS = 512
PARAMS = 151001088


def steps_of(key, dims, pieces, smallest, high):
    level, own = 1.0, jax.random.fold_in(key, 6)
    for dim, shards_of in pieces:
        draws = jnp.exp(jax.random.uniform(jax.random.fold_in(own, dim), (shards_of,), jnp.float32, smallest / len(pieces), high / len(pieces)))
        level = level * jnp.repeat(draws, dims[dim] // shards_of).reshape([-1 if axis == dim else 1 for axis in range(len(dims))])
    return level


def bell_draw(rng, dims, scale, reach, split=(), held_as=jnp.bfloat16):
    drawn = jax.random.normal(rng, dims, jnp.float32) * scale
    if len(split) > 0:
        drawn = steps_of(rng, dims, split, -0.22, 0.18) * drawn
    return jnp.clip(drawn, min=-reach, max=reach).astype(held_as)


def setup_inputs(seed: int = 0) -> dict:
    arg_keys = jax.random.split(jax.random.key(seed), 7)
    return {
        "x_fwd": bell_draw(arg_keys[0], (TOKENS, D), 1.0, 6.0, ((0, 8), (1, 4))),
        "x_bwd": bell_draw(arg_keys[1], (TOKENS, D), 1.0, 6.0, ((0, 8), (1, 4))),
        "grad_out": bell_draw(arg_keys[2], (TOKENS, D), 0.25, 1.5, ((0, 8), (1, 4))),
        "gain": jnp.clip(1.0 + 0.18 * jax.random.normal(arg_keys[3], (D,), jnp.float32), 0.1, 1.9),
        "w_up": bell_draw(arg_keys[4], (D, FF), D ** -0.5, 0.078125, ((0, 4), (1, 8))),
        "w_down": bell_draw(arg_keys[5], (FF, D), FF ** -0.5, 0.0546875, ((0, 8), (1, 4))),
    }


eps = 1e-06
clip_share = 0.25

def erf_gelu(value):
    return 0.5 * value * (1.0 + lax.erf(value * 0.7071067811865476))

def gelu_slope(value):
    return 0.5 * (1.0 + lax.erf(value * 0.7071067811865476)) + value * jnp.exp(-0.5 * value * value) * 0.3989422804014327

def normalize(tokens):
    values = tokens.astype(jnp.float32)
    width = values.shape[-1]
    centre = lax.optimization_barrier(jnp.sum(values, -1, keepdims=True)) / width
    spread = lax.optimization_barrier(jnp.sum(values * values, -1, keepdims=True)) / width - centre * centre
    inv_scale = lax.rsqrt(spread + eps)
    return ((values - centre) * inv_scale, inv_scale)

def reference(x_fwd, x_bwd, grad_out, gain, w_up, w_down):
    centred_a, _ = normalize(x_fwd)
    normed_a = (centred_a * gain).astype(jnp.bfloat16)
    pre_a = jnp.dot(normed_a, w_up, preferred_element_type=jnp.float32)
    hidden_a = erf_gelu(pre_a).astype(jnp.bfloat16)
    y_fwd = (x_fwd.astype(jnp.float32) + jnp.dot(hidden_a, w_down, preferred_element_type=jnp.float32)).astype(jnp.bfloat16)
    centred_b, inv_scale = normalize(x_bwd)
    normed_b = (centred_b * gain).astype(jnp.bfloat16)
    pre_b = jnp.dot(normed_b, w_up, preferred_element_type=jnp.float32)
    hidden_b = erf_gelu(pre_b).astype(jnp.bfloat16)
    grad_hidden = jnp.dot(grad_out, w_down.T, preferred_element_type=jnp.float32)
    grad_pre = (grad_hidden * gelu_slope(pre_b)).astype(jnp.bfloat16)
    g_down = jnp.dot(hidden_b.T, grad_out, preferred_element_type=jnp.float32)
    g_up = jnp.dot(normed_b.T, grad_pre, preferred_element_type=jnp.float32)
    grad_normed = jnp.dot(grad_pre, w_up.T, preferred_element_type=jnp.float32)
    g_gain = lax.optimization_barrier(jnp.sum(grad_normed * centred_b, 0))
    scaled = grad_normed * gain
    width = scaled.shape[-1]
    first = lax.optimization_barrier(jnp.sum(scaled, -1, keepdims=True)) / width
    second = lax.optimization_barrier(jnp.sum(scaled * centred_b, -1, keepdims=True)) / width
    dx_bwd = (grad_out.astype(jnp.float32) + inv_scale * (scaled - first - centred_b * second)).astype(jnp.bfloat16)
    total = jnp.sum(g_up * g_up) + jnp.sum(g_down * g_down) + jnp.sum(g_gain * g_gain)
    norm_value = jnp.sqrt(total)
    grad_rms = norm_value / math.sqrt(PARAMS)
    factor = jnp.minimum(1.0, clip_share * math.sqrt(PARAMS) / norm_value)
    return (y_fwd, dx_bwd, g_up * factor, g_down * factor, g_gain * factor, grad_rms)
```

```python
import functools
import math

import jax
import jax.numpy as jnp
from jax import lax
from jax.experimental import pallas as pl
from jax.experimental.pallas import tpu as pltpu
from jax.sharding import PartitionSpec as P

D = 6144
FF = 12288


eps = 1e-06
clip_share = 0.25


def erf_gelu(value):
    return 0.5 * value * (1.0 + lax.erf(value * 0.7071067811865476))


def gelu_slope(value):
    return (
        0.5 * (1.0 + lax.erf(value * 0.7071067811865476))
        + value * jnp.exp(-0.5 * value * value) * 0.3989422804014327
    )


def contract(left, right, left_dim, right_dim):
    return lax.dot_general(
        left, right, (((left_dim,), (right_dim,)), ((), ())), preferred_element_type=jnp.float32
    )


def row_sums(tokens):
    values = tokens.astype(jnp.float32)
    return (jnp.sum(values, -1), jnp.sum(values * values, -1))


def normalize(tokens, first, second):
    values = tokens.astype(jnp.float32)
    centre = first / D
    spread = second / D - centre * centre
    inv_scale = lax.rsqrt(spread + eps)
    return ((values - centre[:, None]) * inv_scale[:, None], inv_scale)


def up_both(normed_a, normed_b, w_up):
    full_a, full_b = (
        lax.all_gather(normed_a, "row", axis=0, tiled=True),
        lax.all_gather(normed_b, "row", axis=0, tiled=True),
    )
    width = w_up.shape[1]
    summed = lax.psum_scatter(
        jnp.concatenate(
            [
                jnp.dot(full_a, w_up, preferred_element_type=jnp.float32),
                jnp.dot(full_b, w_up, preferred_element_type=jnp.float32),
            ],
            1,
        ),
        "col",
        scatter_dimension=0,
        tiled=True,
    )
    return (summed[:, :width], summed[:, width:], full_b)


def on_device(x_fwd, x_bwd, grad_out, gain, w_up, w_down):
    first_a, second_a = row_sums(x_fwd)
    first_b, second_b = row_sums(x_bwd)
    first_a, second_a, first_b, second_b = lax.psum((first_a, second_a, first_b, second_b), "col")
    centred_a, _ = normalize(x_fwd, first_a, second_a)
    centred_b, inv_scale = normalize(x_bwd, first_b, second_b)
    normed_a = (centred_a * gain).astype(jnp.bfloat16)
    normed_b = (centred_b * gain).astype(jnp.bfloat16)
    pre_a, pre_b, normed_full = up_both(normed_a, normed_b, w_up)
    hidden_a = erf_gelu(pre_a).astype(jnp.bfloat16)
    output_part = jnp.dot(
        lax.all_gather(hidden_a, "col", axis=0, tiled=True),
        w_down,
        preferred_element_type=jnp.float32,
    )
    output_sum = lax.psum_scatter(output_part, "row", scatter_dimension=0, tiled=True)
    y_fwd = (x_fwd.astype(jnp.float32) + output_sum).astype(jnp.bfloat16)
    hidden_b = erf_gelu(pre_b).astype(jnp.bfloat16)
    grad_full = lax.all_gather(grad_out, "row", axis=0, tiled=True)
    grad_hidden = lax.psum_scatter(
        contract(grad_full, w_down, 1, 1), "col", scatter_dimension=0, tiled=True
    )
    grad_pre = (grad_hidden * gelu_slope(pre_b)).astype(jnp.bfloat16)
    hidden_piece = lax.all_gather(hidden_b, "col", axis=0, tiled=True)
    pre_piece = lax.all_gather(grad_pre, "col", axis=0, tiled=True)
    down_total = contract(hidden_piece, grad_full, 0, 0)
    up_total = contract(normed_full, pre_piece, 0, 0)
    input_total = contract(pre_piece, w_up, 1, 1)
    grad_normed = lax.psum_scatter(input_total, "row", scatter_dimension=0, tiled=True)
    scaled = grad_normed * gain
    first_back = jnp.sum(scaled, -1)
    second_back = jnp.sum(scaled * centred_b, -1)
    first_back, second_back = lax.psum((first_back, second_back), "col")
    dx_bwd = (
        grad_out.astype(jnp.float32)
        + inv_scale[:, None]
        * (scaled - first_back[:, None] / D - centred_b * (second_back[:, None] / D))
    ).astype(jnp.bfloat16)
    gain_part = jnp.sum(grad_normed * centred_b, 0)
    weight_squares = jnp.sum(up_total * up_total) + jnp.sum(down_total * down_total)
    g_gain = lax.psum(gain_part, "row")
    first_row = (lax.axis_index("row") == 0).astype(jnp.float32)
    total = lax.psum(weight_squares + first_row * jnp.sum(g_gain * g_gain), ("row", "col"))
    param_count = 2 * D * FF + D
    norm_value = jnp.sqrt(total)
    grad_rms = norm_value / math.sqrt(param_count)
    factor = jnp.minimum(1.0, clip_share * math.sqrt(param_count) / norm_value)
    return (y_fwd, dx_bwd, up_total * factor, down_total * factor, g_gain * factor, grad_rms)


MESH = pl.DeviceIdType.MESH
VMEM = pl.BlockSpec(memory_space=pltpu.VMEM)
F32 = jnp.float32
BF16 = jnp.bfloat16
DMA = pltpu.SemaphoreType.DMA
GRANT = 60 * 1024 * 1024


def greet(peers):
    barrier = pltpu.get_barrier_semaphore()
    for peer in peers:
        pl.semaphore_signal(barrier, inc=1, device_id=peer, device_id_type=MESH)
    pl.semaphore_wait(barrier, len(peers))


def send(src, dst, send_sem, recv_sem, peer):
    return pltpu.make_async_remote_copy(
        src_ref=src, dst_ref=dst, send_sem=send_sem, recv_sem=recv_sem,
        device_id=peer, device_id_type=MESH,
    )


def arrived(ref, sem, peer):
    pltpu.make_async_remote_copy(
        src_ref=ref, dst_ref=ref, send_sem=sem, recv_sem=sem,
        device_id=peer, device_id_type=MESH,
    ).wait_recv()


def greet_line(line, chip, chips, others):
    barrier = pltpu.get_barrier_semaphore()
    for peer in others:
        pl.semaphore_signal(barrier, inc=1, device_id=peer, device_id_type=MESH)

    @pl.when(chip > 0)
    def _():
        pl.semaphore_signal(barrier, inc=1, device_id=line(-1), device_id_type=MESH)

    @pl.when(chip < chips - 1)
    def _():
        pl.semaphore_signal(barrier, inc=1, device_id=line(1), device_id_type=MESH)

    beside = jnp.minimum(chip, 1) + jnp.minimum(chips - 1 - chip, 1)
    pl.semaphore_wait(barrier, len(others) + beside)


def normal_of(values, stats, at, width):
    centre = stats[:, at : at + 1] / width
    spread = stats[:, at + 1 : at + 2] / width - centre * centre
    inv = lax.rsqrt(spread + eps)
    return (values - centre) * inv, inv


def lanes_of(columns):
    rows = columns[0].shape[0]
    lane = lax.broadcasted_iota(jnp.int32, (rows, 128), 1)
    out = jnp.zeros((rows, 128), F32)
    for i, column in enumerate(columns):
        out = jnp.where(lane == i, column, out)
    return out


def gather_kernel(R, C, width, xa, xb, go, gain, full, stats, st_own, st_in,
                  st_send, st_recv, s_right, s_left, s_sib, recv):
    row, col = lax.axis_index("row"), lax.axis_index("col")
    chips = R // 2
    chip, core = row // 2, row % 2
    sib = {"row": row + 1 - 2 * core, "col": col}

    def line(step):
        return {"row": row + 2 * step, "col": col}

    cols = [{"row": row, "col": (col + i) % C} for i in range(1, C)]
    greet_line(line, chip, chips, cols + [sib])

    def spread(j, owner, slot, src, to_right, to_left):
        dst = full.at[j, owner]
        out = [(None, send(src, dst, s_sib.at[j, slot], recv.at[j, owner], sib))]
        if to_right:
            out.append((chip < chips - 1,
                        send(src, dst, s_right.at[j, slot], recv.at[j, owner], line(1))))
        if to_left:
            out.append((chip > 0,
                        send(src, dst, s_left.at[j, slot], recv.at[j, owner], line(-1))))
        return out

    def start(copies):
        for cond, copy in copies[::-1]:
            if cond is None:
                copy.start()
            else:
                pl.when(cond)(copy.start)

    def finish(copies):
        for cond, copy in copies:
            if cond is None:
                copy.wait_send()
            else:
                pl.when(cond)(copy.wait_send)

    own = {2: spread(2, row, 0, go, True, True)}
    start(own[2])
    a, b = xa[...].astype(F32), xb[...].astype(F32)
    sums = []
    for v in (a, b):
        sums += [jnp.sum(v, 1, keepdims=True), jnp.sum(v * v, 1, keepdims=True)]
    st_own[...] = lanes_of(sums)
    st_copies = [send(st_own, st_in.at[i], st_send.at[i], st_recv.at[i], p)
                 for i, p in enumerate(cols)]
    for copy in st_copies:
        copy.start()
    full[2, row] = go[...]
    for copy in st_copies:
        copy.wait()
    total = st_own[...]
    for i in range(C - 1):
        total = total + st_in[i]
    stats[...] = total
    for j, x, at in ((1, xb, 2), (0, xa, 0)):
        hat, _ = normal_of(x[...].astype(F32), total, at, width)
        full[j, row] = (hat * gain[...]).astype(BF16)
        own[j] = spread(j, row, 0, full.at[j, row], True, True)
        start(own[j])
    for step in range(1, chips):
        for j in (2, 1, 0):
            for sign in (-1, 1):
                ok = chip >= step if sign < 0 else chip + step < chips

                @pl.when(ok)
                def _():
                    owner = row + 2 * sign * step
                    arrived(full.at[j, owner], recv.at[j, owner], line(sign))
                    slot = step if sign < 0 else chips - 1 + step
                    start(spread(j, owner, slot, full.at[j, owner], sign < 0, sign > 0))
    for j in (2, 1, 0):
        finish(own[j])
        for chip_of in range(chips):
            owner = 2 * chip_of + 1 - core
            arrived(full.at[j, owner], recv.at[j, owner], sib)
    for step in range(1, chips):
        for j in (2, 1, 0):
            for sign in (-1, 1):
                ok = chip >= step if sign < 0 else chip + step < chips

                @pl.when(ok)
                def _():
                    owner = row + 2 * sign * step
                    slot = step if sign < 0 else chips - 1 + step
                    finish(spread(j, owner, slot, full.at[j, owner], sign < 0, sign > 0))


def gather_rows(R, C, width, x_fwd, x_bwd, grad_out, gain):
    rows, columns = x_fwd.shape
    slots = 2 * (R // 2) - 1
    return pl.pallas_call(
        functools.partial(gather_kernel, R, C, width),
        out_shape=(jax.ShapeDtypeStruct((3, R, rows, columns), BF16),
                   jax.ShapeDtypeStruct((rows, 128), F32)),
        in_specs=[VMEM] * 4,
        out_specs=(VMEM, VMEM),
        scratch_shapes=[
            pltpu.VMEM((rows, 128), F32), pltpu.VMEM((C - 1, rows, 128), F32),
            DMA((C - 1,)), DMA((C - 1,)),
            DMA((3, slots)), DMA((3, slots)), DMA((3, slots)), DMA((3, R)),
        ],
        compiler_params=pltpu.CompilerParams(
            collective_id=0, has_side_effects=True, vmem_limit_bytes=GRANT),
        cost_estimate=pl.CostEstimate(flops=10**9, bytes_accessed=10**7, transcendentals=0),
    )(x_fwd, x_bwd, grad_out, gain)


def middle_kernel(full, w_up, w_down, out, out_send, buf, inb, own, sem_s, sem_r, g_s, g_r):
    row, col = lax.axis_index("row"), lax.axis_index("col")
    flip_x = col + 1 - 2 * (col % 2)
    flip_y = (col + 2) % 4
    diag = 3 - col
    peer_x, peer_y = {"row": row, "col": flip_x}, {"row": row, "col": flip_y}
    greet([peer_x, peer_y])
    tokens, wide = out.shape[2], out.shape[3]
    half = wide // 2
    tile = half // 2

    def part(j, q, put):
        @pl.loop(0, wide // tile)
        def _(t):
            at = pl.ds(pl.multiple_of(t * tile, tile), tile)
            left = full[j, q]
            if j == 2:
                piece = lax.dot_general(left, w_down[at, :], (((1,), (1,)), ((), ())),
                                        preferred_element_type=F32)
            else:
                piece = jnp.dot(left, w_up[:, at], preferred_element_type=F32)
            put(t, piece)

    def into(j, base):
        def put(t, piece):
            buf[j, base + t // 2, :, pl.ds(pl.multiple_of((t % 2) * tile, tile), tile)] = piece
        return put

    def keep(j):
        def put(t, piece):
            own[j, t // 2, :, pl.ds(pl.multiple_of((t % 2) * tile, tile), tile)] = piece
        return put

    target = (peer_x, peer_y, peer_x, peer_x, peer_y, peer_y)

    def copy(j, s):
        return send(buf.at[j, s], inb.at[j, s], sem_s.at[j, s], sem_r.at[j, s], target[s])

    def products(j):
        part(j, diag, into(j, 0))
        copy(j, 0).start()
        copy(j, 1).start()
        part(j, flip_x, into(j, 2))
        copy(j, 2).start()
        part(j, flip_y, into(j, 4))
        copy(j, 5).start()
        part(j, col, keep(j))

    def transit(j):
        copy(j, 0).wait_recv()
        buf[j, 4] = buf[j, 4] + inb[j, 0]
        copy(j, 4).start()
        copy(j, 1).wait_recv()
        buf[j, 3] = buf[j, 3] + inb[j, 1]
        copy(j, 3).start()

    def total(j):
        for s in range(2, 6):
            copy(j, s).wait_recv()

    def summed(j, h, at):
        return own[j, h, at, :] + inb[j, 2 + h, at, :] + inb[j, 4 + h, at, :]

    chunk = 16

    def over(body):
        @pl.loop(0, tokens // chunk)
        def _(i):
            for h in range(2):
                body(h, pl.ds(pl.multiple_of(i * chunk, chunk), chunk))

    def first(k, which):
        peer = (peer_x, peer_y)[which]
        return send(out_send.at[k], out.at[k, col], g_s.at[k, which], g_r.at[k, which], peer)

    def relay(k, which):
        owner = (flip_x, flip_y)[which]
        ref = out.at[k, owner, :, pl.ds(which * half, half)]
        return send(ref, ref, g_s.at[k, 2 + which], g_r.at[k, 2 + which], (peer_y, peer_x)[which])

    def publish(k):
        first(k, 0).start()
        first(k, 1).start()

    def pass_on(k):
        first(k, 0).wait_recv()
        relay(k, 0).start()
        first(k, 1).wait_recv()
        relay(k, 1).start()

    products(2)
    products(1)
    transit(2)
    products(0)
    transit(1)
    total(2)
    total(1)

    def backward(h, at):
        v = summed(1, h, at)
        phi = 0.5 * (1.0 + lax.erf(v * 0.7071067811865476))
        g = summed(2, h, at)
        slope = phi + v * jnp.exp(-0.5 * v * v) * 0.3989422804014327
        out_send[1, at, h * half : (h + 1) * half] = (v * phi).astype(BF16)
        out_send[2, at, h * half : (h + 1) * half] = (g * slope).astype(BF16)

    over(backward)
    transit(0)
    publish(2)
    publish(1)
    total(0)

    def forward(h, at):
        v = summed(0, h, at)
        out_send[0, at, h * half : (h + 1) * half] = (
            0.5 * v * (1.0 + lax.erf(v * 0.7071067811865476))).astype(BF16)

    over(forward)
    publish(0)
    for k in (2, 1, 0):
        out[k, col] = out_send[k]
        pass_on(k)
    for k in (2, 1, 0):
        relay(k, 0).wait_send()
        relay(k, 1).wait_send()
        first(k, 0).wait_send()
        first(k, 1).wait_send()
        for which in (0, 1):
            ref = out.at[k, diag, :, pl.ds(which * half, half)]
            arrived(ref, g_r.at[k, 2 + which], (peer_y, peer_x)[which])
        for s in range(6):
            copy(k, s).wait_send()


def middle(full, w_up, w_down):
    _, C, tokens, _ = full.shape
    wide = w_up.shape[1]
    half = wide // 2
    return pl.pallas_call(
        middle_kernel,
        out_shape=jax.ShapeDtypeStruct((3, C, tokens, wide), BF16),
        in_specs=[VMEM] * 3,
        out_specs=VMEM,
        scratch_shapes=[
            pltpu.VMEM((3, tokens, wide), BF16),
            pltpu.VMEM((3, 6, tokens, half), F32), pltpu.VMEM((3, 6, tokens, half), F32),
            pltpu.VMEM((3, 2, tokens, half), F32),
            DMA((3, 6)), DMA((3, 6)), DMA((3, 4)), DMA((3, 4)),
        ],
        compiler_params=pltpu.CompilerParams(
            collective_id=1, has_side_effects=True, vmem_limit_bytes=GRANT),
        cost_estimate=pl.CostEstimate(flops=10**10, bytes_accessed=10**7, transcendentals=0),
    )(full, w_up, w_down)


def scatter_kernel(R, hidden, w_up, w_down, out, part, from_sib, from_left, from_right,
                   sib_s, sib_r, right_s, left_s, left_r, right_r):
    row, col = lax.axis_index("row"), lax.axis_index("col")
    chips = R // 2
    chip, core = row // 2, row % 2
    sib = {"row": row + 1 - 2 * core, "col": col}

    def line(step):
        return {"row": row + 2 * step, "col": col}

    greet_line(line, chip, chips, [sib])
    rows, wide = out.shape[1], out.shape[2]
    tile = wide // 4
    order = []
    low, high = 0, chips - 1
    while low <= high:
        order.append(high)
        if low < high:
            order.append(low)
        low, high = low + 1, high - 1

    def to_sib(j, z):
        return send(part.at[j, z, 1 - core], from_sib.at[j, z], sib_s.at[j, z], sib_r.at[j, z], sib)

    def to_right(j, z):
        return send(part.at[j, z, core], from_left.at[j, z], right_s.at[j, z], left_r.at[j, z], line(1))

    def to_left(j, z):
        return send(part.at[j, z, core], from_right.at[j, z], left_s.at[j, z], right_r.at[j, z], line(-1))

    def product(j, z):
        @pl.loop(0, wide // tile)
        def _(t):
            at = pl.ds(pl.multiple_of(t * tile, tile), tile)
            left = hidden[2 * j, pl.ds(z * 2 * rows, 2 * rows), :]
            if j == 0:
                piece = jnp.dot(left, w_down[:, at], preferred_element_type=F32)
            else:
                piece = lax.dot_general(left, w_up[at, :], (((1,), (1,)), ((), ())),
                                        preferred_element_type=F32)
            part[j, z, 0, :, at] = piece[:rows]
            part[j, z, 1, :, at] = piece[rows:]
        to_sib(j, z).start()

    def onward(j, z):
        to_sib(j, z).wait_recv()
        part[j, z, core] = part[j, z, core] + from_sib[j, z]

        @pl.when(z > chip)
        def _():
            @pl.when(chip > 0)
            def _():
                to_right(j, z).wait_recv()
                part[j, z, core] = part[j, z, core] + from_left[j, z]

            to_right(j, z).start()

        @pl.when(z < chip)
        def _():
            @pl.when(chip < chips - 1)
            def _():
                to_left(j, z).wait_recv()
                part[j, z, core] = part[j, z, core] + from_right[j, z]

            to_left(j, z).start()

    for j in (0, 1):
        for z in order:
            product(j, z)
    for j in (0, 1):
        for z in order:
            onward(j, z)
    for j in (0, 1):
        out[j] = part[j, chip, core]

        @pl.when(chip > 0)
        def _():
            to_right(j, chip).wait_recv()
            out[j] = out[j] + from_left[j, chip]

        @pl.when(chip < chips - 1)
        def _():
            to_left(j, chip).wait_recv()
            out[j] = out[j] + from_right[j, chip]

    for j in (0, 1):
        for z in range(chips):
            to_sib(j, z).wait_send()
            pl.when(z > chip)(to_right(j, z).wait_send)
            pl.when(z < chip)(to_left(j, z).wait_send)


def scatter_rows(R, hidden, w_up, w_down):
    tokens, wide = hidden.shape[1], w_up.shape[0]
    rows, chips = tokens // R, R // 2
    block = (2, chips, rows, wide)
    return pl.pallas_call(
        functools.partial(scatter_kernel, R),
        out_shape=jax.ShapeDtypeStruct((2, rows, wide), F32),
        in_specs=[VMEM] * 3,
        out_specs=VMEM,
        scratch_shapes=[pltpu.VMEM((2, chips, 2, rows, wide), F32)]
        + [pltpu.VMEM(block, F32)] * 3 + [DMA((2, chips))] * 6,
        compiler_params=pltpu.CompilerParams(
            collective_id=2, has_side_effects=True, vmem_limit_bytes=GRANT),
        cost_estimate=pl.CostEstimate(flops=10**10, bytes_accessed=10**7, transcendentals=0),
    )(hidden, w_up, w_down)


def final_kernel(R, C, width, gn, xb, go, gain, stats, squares, dx, g_gain, total,
                 st_own, st_in, gp_own, gp_in, tt_own, tt_in,
                 st_s, st_r, gp_s, gp_r, tt_s, tt_r):
    row, col = lax.axis_index("row"), lax.axis_index("col")
    cols = [{"row": row, "col": (col + i) % C} for i in range(1, C)]
    rows = [{"row": (row + i) % R, "col": col} for i in range(1, R)]
    greet(cols + rows)
    hat, inv = normal_of(xb[...].astype(F32), stats[...], 2, width)
    grad = gn[...]
    scaled = grad * gain[...]
    st_own[...] = lanes_of([jnp.sum(scaled, 1, keepdims=True), jnp.sum(scaled * hat, 1, keepdims=True)])
    first = [send(st_own, st_in.at[i], st_s.at[i], st_r.at[i], p) for i, p in enumerate(cols)]
    for copy in first:
        copy.start()
    wide = grad.shape[1]
    gp_own[:, :wide] = jnp.broadcast_to(jnp.sum(grad * hat, 0, keepdims=True), (8, wide))
    gp_own[:, wide:] = squares[...]
    gp_in[row] = gp_own[...]
    second = [send(gp_own, gp_in.at[row], gp_s.at[i], gp_r.at[i], p) for i, p in enumerate(rows)]
    for copy in second:
        copy.start()
    for copy in second:
        copy.wait()
    gains = gp_in[0]
    for i in range(1, R):
        gains = gains + gp_in[i]
    gained = gains[:, :wide]
    g_gain[...] = gained
    tt_own[...] = gains[:, wide:] + jnp.sum(gained * gained, 1, keepdims=True)
    tt_in[col] = tt_own[...]
    third = [send(tt_own, tt_in.at[col], tt_s.at[i], tt_r.at[i], p) for i, p in enumerate(cols)]
    for copy in third:
        copy.start()
    for copy in first:
        copy.wait()
    sums = st_own[...]
    for i in range(C - 1):
        sums = sums + st_in[i]
    c1, c2 = sums[:, 0:1] / width, sums[:, 1:2] / width
    dx[...] = (go[...].astype(F32) + inv * (scaled - c1 - hat * c2)).astype(BF16)
    for copy in third:
        copy.wait()
    whole = tt_in[0]
    for i in range(1, C):
        whole = whole + tt_in[i]
    total[...] = whole


def final(R, C, width, gn, x_bwd, grad_out, gain, stats, squares):
    rows, wide = gn.shape
    return pl.pallas_call(
        functools.partial(final_kernel, R, C, width),
        out_shape=(jax.ShapeDtypeStruct((rows, wide), BF16),
                   jax.ShapeDtypeStruct((8, wide), F32),
                   jax.ShapeDtypeStruct((8, 128), F32)),
        in_specs=[VMEM] * 6,
        out_specs=(VMEM, VMEM, VMEM),
        scratch_shapes=[
            pltpu.VMEM((rows, 128), F32), pltpu.VMEM((C - 1, rows, 128), F32),
            pltpu.VMEM((8, wide + 128), F32), pltpu.VMEM((R, 8, wide + 128), F32),
            pltpu.VMEM((8, 128), F32), pltpu.VMEM((C, 8, 128), F32),
            DMA((C - 1,)), DMA((C - 1,)), DMA((R - 1,)), DMA((R - 1,)), DMA((C - 1,)), DMA((C - 1,)),
        ],
        compiler_params=pltpu.CompilerParams(
            collective_id=3, has_side_effects=True, vmem_limit_bytes=GRANT),
        cost_estimate=pl.CostEstimate(flops=10**9, bytes_accessed=10**7, transcendentals=0),
    )(gn, x_bwd, grad_out, gain, stats, squares)


def with_kernels(R, C):
    def step(x_fwd, x_bwd, grad_out, gain, w_up, w_down):
        rows, columns = x_fwd.shape
        tokens = rows * R
        width = columns * C
        gain_row = gain.reshape(1, columns)
        full, stats = gather_rows(R, C, width, x_fwd, x_bwd, grad_out, gain_row)
        acts = middle(full.reshape(3, C, tokens // C, columns), w_up, w_down)
        acts = acts.reshape(3, tokens, w_up.shape[1])
        full = full.reshape(3, tokens, columns)
        sums = scatter_rows(R, acts, w_up, w_down)
        y_fwd = (x_fwd.astype(F32) + sums[0]).astype(BF16)
        down_total = contract(acts[1], full[2], 0, 0)
        up_total = contract(full[1], acts[2], 0, 0)
        squares = jnp.sum(up_total * up_total) + jnp.sum(down_total * down_total)
        dx, g_gain, total = final(R, C, width, sums[1], x_bwd, grad_out, gain_row, stats,
                                  jnp.broadcast_to(squares, (8, 128)))
        param_count = 2 * width * w_up.shape[1] * R + width
        norm_value = jnp.sqrt(total[0, 0])
        grad_rms = norm_value / math.sqrt(param_count)
        factor = jnp.minimum(1.0, clip_share * math.sqrt(param_count) / norm_value)
        return (y_fwd, dx, up_total * factor, down_total * factor, g_gain[0] * factor, grad_rms)

    return step


def solution(mesh):
    placed = (
        P("row", "col"),
        P("row", "col"),
        P("row", "col"),
        P("col"),
        P("col", "row"),
        P("row", "col"),
    )
    R, C = mesh.shape["row"], mesh.shape["col"]
    body = with_kernels(R, C) if C == 4 and R % 2 == 0 else on_device
    return jax.shard_map(
        body,
        mesh=mesh,
        in_specs=placed,
        out_specs=(
            P("row", "col"),
            P("row", "col"),
            P("col", "row"),
            P("row", "col"),
            P("col"),
            P(),
        ),
        check_vma=False,
    )
```

```python
import functools
import math

import jax
import jax.numpy as jnp
from jax import lax
from jax.experimental import pallas as pl
from jax.experimental.pallas import tpu as pltpu
from jax.sharding import PartitionSpec as P

D = 6144
FF = 12288


eps = 1e-06
clip_share = 0.25


def erf_gelu(value):
    return 0.5 * value * (1.0 + lax.erf(value * 0.7071067811865476))


def gelu_slope(value):
    return (
        0.5 * (1.0 + lax.erf(value * 0.7071067811865476))
        + value * jnp.exp(-0.5 * value * value) * 0.3989422804014327
    )


def contract(left, right, left_dim, right_dim):
    return lax.dot_general(
        left, right, (((left_dim,), (right_dim,)), ((), ())), preferred_element_type=jnp.float32
    )


def row_sums(tokens):
    values = tokens.astype(jnp.float32)
    return (jnp.sum(values, -1), jnp.sum(values * values, -1))


def normalize(tokens, first, second):
    values = tokens.astype(jnp.float32)
    centre = first / D
    spread = second / D - centre * centre
    inv_scale = lax.rsqrt(spread + eps)
    return ((values - centre[:, None]) * inv_scale[:, None], inv_scale)


def up_both(normed_a, normed_b, w_up):
    full_a, full_b = (
        lax.all_gather(normed_a, "row", axis=0, tiled=True),
        lax.all_gather(normed_b, "row", axis=0, tiled=True),
    )
    width = w_up.shape[1]
    summed = lax.psum_scatter(
        jnp.concatenate(
            [
                jnp.dot(full_a, w_up, preferred_element_type=jnp.float32),
                jnp.dot(full_b, w_up, preferred_element_type=jnp.float32),
            ],
            1,
        ),
        "col",
        scatter_dimension=0,
        tiled=True,
    )
    return (summed[:, :width], summed[:, width:], full_b)


def on_device(x_fwd, x_bwd, grad_out, gain, w_up, w_down):
    first_a, second_a = row_sums(x_fwd)
    first_b, second_b = row_sums(x_bwd)
    first_a, second_a, first_b, second_b = lax.psum((first_a, second_a, first_b, second_b), "col")
    centred_a, _ = normalize(x_fwd, first_a, second_a)
    centred_b, inv_scale = normalize(x_bwd, first_b, second_b)
    normed_a = (centred_a * gain).astype(jnp.bfloat16)
    normed_b = (centred_b * gain).astype(jnp.bfloat16)
    pre_a, pre_b, normed_full = up_both(normed_a, normed_b, w_up)
    hidden_a = erf_gelu(pre_a).astype(jnp.bfloat16)
    output_part = jnp.dot(
        lax.all_gather(hidden_a, "col", axis=0, tiled=True),
        w_down,
        preferred_element_type=jnp.float32,
    )
    output_sum = lax.psum_scatter(output_part, "row", scatter_dimension=0, tiled=True)
    y_fwd = (x_fwd.astype(jnp.float32) + output_sum).astype(jnp.bfloat16)
    hidden_b = erf_gelu(pre_b).astype(jnp.bfloat16)
    grad_full = lax.all_gather(grad_out, "row", axis=0, tiled=True)
    grad_hidden = lax.psum_scatter(
        contract(grad_full, w_down, 1, 1), "col", scatter_dimension=0, tiled=True
    )
    grad_pre = (grad_hidden * gelu_slope(pre_b)).astype(jnp.bfloat16)
    hidden_piece = lax.all_gather(hidden_b, "col", axis=0, tiled=True)
    pre_piece = lax.all_gather(grad_pre, "col", axis=0, tiled=True)
    down_total = contract(hidden_piece, grad_full, 0, 0)
    up_total = contract(normed_full, pre_piece, 0, 0)
    input_total = contract(pre_piece, w_up, 1, 1)
    grad_normed = lax.psum_scatter(input_total, "row", scatter_dimension=0, tiled=True)
    scaled = grad_normed * gain
    first_back = jnp.sum(scaled, -1)
    second_back = jnp.sum(scaled * centred_b, -1)
    first_back, second_back = lax.psum((first_back, second_back), "col")
    dx_bwd = (
        grad_out.astype(jnp.float32)
        + inv_scale[:, None]
        * (scaled - first_back[:, None] / D - centred_b * (second_back[:, None] / D))
    ).astype(jnp.bfloat16)
    gain_part = jnp.sum(grad_normed * centred_b, 0)
    weight_squares = jnp.sum(up_total * up_total) + jnp.sum(down_total * down_total)
    g_gain = lax.psum(gain_part, "row")
    first_row = (lax.axis_index("row") == 0).astype(jnp.float32)
    total = lax.psum(weight_squares + first_row * jnp.sum(g_gain * g_gain), ("row", "col"))
    param_count = 2 * D * FF + D
    norm_value = jnp.sqrt(total)
    grad_rms = norm_value / math.sqrt(param_count)
    factor = jnp.minimum(1.0, clip_share * math.sqrt(param_count) / norm_value)
    return (y_fwd, dx_bwd, up_total * factor, down_total * factor, g_gain * factor, grad_rms)


MESH = pl.DeviceIdType.MESH
VMEM = pl.BlockSpec(memory_space=pltpu.VMEM)
F32 = jnp.float32
BF16 = jnp.bfloat16
DMA = pltpu.SemaphoreType.DMA
GRANT = 60 * 1024 * 1024


def greet(peers):
    barrier = pltpu.get_barrier_semaphore()
    for peer in peers:
        pl.semaphore_signal(barrier, inc=1, device_id=peer, device_id_type=MESH)
    pl.semaphore_wait(barrier, len(peers))


def send(src, dst, send_sem, recv_sem, peer):
    return pltpu.make_async_remote_copy(
        src_ref=src, dst_ref=dst, send_sem=send_sem, recv_sem=recv_sem,
        device_id=peer, device_id_type=MESH,
    )


def arrived(ref, sem, peer):
    pltpu.make_async_remote_copy(
        src_ref=ref, dst_ref=ref, send_sem=sem, recv_sem=sem,
        device_id=peer, device_id_type=MESH,
    ).wait_recv()


def greet_line(line, chip, chips, others):
    barrier = pltpu.get_barrier_semaphore()
    for peer in others:
        pl.semaphore_signal(barrier, inc=1, device_id=peer, device_id_type=MESH)

    @pl.when(chip > 0)
    def _():
        pl.semaphore_signal(barrier, inc=1, device_id=line(-1), device_id_type=MESH)

    @pl.when(chip < chips - 1)
    def _():
        pl.semaphore_signal(barrier, inc=1, device_id=line(1), device_id_type=MESH)

    beside = jnp.minimum(chip, 1) + jnp.minimum(chips - 1 - chip, 1)
    pl.semaphore_wait(barrier, len(others) + beside)


def normal_of(values, stats, at, width):
    centre = stats[:, at : at + 1] / width
    spread = stats[:, at + 1 : at + 2] / width - centre * centre
    inv = lax.rsqrt(spread + eps)
    return (values - centre) * inv, inv


def lanes_of(columns):
    rows = columns[0].shape[0]
    lane = lax.broadcasted_iota(jnp.int32, (rows, 128), 1)
    out = jnp.zeros((rows, 128), F32)
    for i, column in enumerate(columns):
        out = jnp.where(lane == i, column, out)
    return out


def layer_kernel(R, C, width, xa, xb, go, gain, w_up_hbm, w_down_hbm, full, stats, acts, sums,
                 w_up, w_down, st_own, st_in, out_send, buf, inb, own,
                 part, from_sib, from_left, from_right,
                 w_sem, st_send, st_recv, s_right, s_left, s_sib, recv, sem_s, sem_r, g_s, g_r,
                 sib_s, sib_r, right_s, left_s, left_r, right_r):
    row, col = lax.axis_index("row"), lax.axis_index("col")
    chips = R // 2
    chip, core = row // 2, row % 2
    sib = {"row": row + 1 - 2 * core, "col": col}

    def line(step):
        return {"row": row + 2 * step, "col": col}

    cols = [{"row": row, "col": (col + i) % C} for i in range(1, C)]
    flip_x = col + 1 - 2 * (col % 2)
    flip_y = (col + 2) % 4
    diag = 3 - col
    peer_x, peer_y = {"row": row, "col": flip_x}, {"row": row, "col": flip_y}
    share = xa.shape[0]
    tokens, wide = out_send.shape[1], out_send.shape[2]
    half = wide // 2
    tile = half // 2
    load_up = pltpu.make_async_copy(w_up_hbm, w_up, w_sem.at[0])
    load_down = pltpu.make_async_copy(w_down_hbm, w_down, w_sem.at[1])
    load_down.start()
    load_up.start()
    greet_line(line, chip, chips, cols + [sib])

    def block(j, owner):
        return full.at[j, pl.ds(owner * share, share), :]

    def spread(j, owner, slot, src, to_right, to_left):
        dst = block(j, owner)
        out = [(None, send(src, dst, s_sib.at[j, slot], recv.at[j, owner], sib))]
        if to_right:
            out.append((chip < chips - 1,
                        send(src, dst, s_right.at[j, slot], recv.at[j, owner], line(1))))
        if to_left:
            out.append((chip > 0,
                        send(src, dst, s_left.at[j, slot], recv.at[j, owner], line(-1))))
        return out

    def start(copies):
        for cond, copy in copies[::-1]:
            if cond is None:
                copy.start()
            else:
                pl.when(cond)(copy.start)

    def finish(copies):
        for cond, copy in copies:
            if cond is None:
                copy.wait_send()
            else:
                pl.when(cond)(copy.wait_send)

    mine = {2: spread(2, row, 0, go, True, True)}
    start(mine[2])
    a, b = xa[...].astype(F32), xb[...].astype(F32)
    moments = []
    for v in (a, b):
        moments += [jnp.sum(v, 1, keepdims=True), jnp.sum(v * v, 1, keepdims=True)]
    st_own[...] = lanes_of(moments)
    st_copies = [send(st_own, st_in.at[i], st_send.at[i], st_recv.at[i], p)
                 for i, p in enumerate(cols)]
    for copy in st_copies:
        copy.start()
    block(2, row)[...] = go[...]
    for copy in st_copies:
        copy.wait()
    total = st_own[...]
    for i in range(C - 1):
        total = total + st_in[i]
    stats[...] = total
    for j, x, at in ((1, xb, 2), (0, xa, 0)):
        hat, _ = normal_of(x[...].astype(F32), total, at, width)
        block(j, row)[...] = (hat * gain[...]).astype(BF16)
        mine[j] = spread(j, row, 0, block(j, row), True, True)
        start(mine[j])

    def relays(j, visit):
        for step in range(1, chips):
            for sign in (-1, 1):
                ok = chip >= step if sign < 0 else chip + step < chips

                @pl.when(ok)
                def _():
                    owner = row + 2 * sign * step
                    slot = step if sign < 0 else chips - 1 + step
                    visit(owner, sign, spread(j, owner, slot, block(j, owner), sign < 0, sign > 0))

    def gathered(j):
        def visit(owner, sign, copies):
            arrived(block(j, owner), recv.at[j, owner], line(sign))
            start(copies)

        relays(j, visit)
        for chip_of in range(chips):
            owner = 2 * chip_of + 1 - core
            arrived(block(j, owner), recv.at[j, owner], sib)

    def multiply(j, q, put):
        @pl.loop(0, wide // tile)
        def _(t):
            at = pl.ds(pl.multiple_of(t * tile, tile), tile)
            left = full[j, pl.ds(q * tokens, tokens), :]
            if j == 2:
                piece = lax.dot_general(left, w_down[at, :], (((1,), (1,)), ((), ())),
                                        preferred_element_type=F32)
            else:
                piece = jnp.dot(left, w_up[:, at], preferred_element_type=F32)
            put(t, piece)

    def into(j, base):
        def put(t, piece):
            buf[j, base + t // 2, :, pl.ds(pl.multiple_of((t % 2) * tile, tile), tile)] = piece
        return put

    def keep(j):
        def put(t, piece):
            own[j, t // 2, :, pl.ds(pl.multiple_of((t % 2) * tile, tile), tile)] = piece
        return put

    target = (peer_x, peer_y, peer_x, peer_x, peer_y, peer_y)

    def hop(j, s):
        return send(buf.at[j, s], inb.at[j, s], sem_s.at[j, s], sem_r.at[j, s], target[s])

    def products(j):
        multiply(j, diag, into(j, 0))
        hop(j, 0).start()
        hop(j, 1).start()
        multiply(j, flip_x, into(j, 2))
        hop(j, 2).start()
        multiply(j, flip_y, into(j, 4))
        hop(j, 5).start()
        multiply(j, col, keep(j))

    def transit(j):
        hop(j, 0).wait_recv()
        buf[j, 4] = buf[j, 4] + inb[j, 0]
        hop(j, 4).start()
        hop(j, 1).wait_recv()
        buf[j, 3] = buf[j, 3] + inb[j, 1]
        hop(j, 3).start()

    def landed(j):
        for s in range(2, 6):
            hop(j, s).wait_recv()

    def summed(j, h, at):
        return own[j, h, at, :] + inb[j, 2 + h, at, :] + inb[j, 4 + h, at, :]

    chunk = 16

    def over(body):
        @pl.loop(0, tokens // chunk)
        def _(i):
            for h in range(2):
                body(h, pl.ds(pl.multiple_of(i * chunk, chunk), chunk))

    def first(k, which):
        peer = (peer_x, peer_y)[which]
        return send(out_send.at[k], acts.at[k, pl.ds(col * tokens, tokens), :], g_s.at[k, which], g_r.at[k, which], peer)

    def relay(k, which):
        owner = (flip_x, flip_y)[which]
        ref = acts.at[k, pl.ds(owner * tokens, tokens), pl.ds(which * half, half)]
        return send(ref, ref, g_s.at[k, 2 + which], g_r.at[k, 2 + which], (peer_y, peer_x)[which])

    def publish(k):
        first(k, 0).start()
        first(k, 1).start()

    def pass_on(k):
        first(k, 0).wait_recv()
        relay(k, 0).start()
        first(k, 1).wait_recv()
        relay(k, 1).start()

    def backward(h, at):
        v = summed(1, h, at)
        phi = 0.5 * (1.0 + lax.erf(v * 0.7071067811865476))
        g = summed(2, h, at)
        slope = phi + v * jnp.exp(-0.5 * v * v) * 0.3989422804014327
        out_send[1, at, h * half : (h + 1) * half] = (v * phi).astype(BF16)
        out_send[2, at, h * half : (h + 1) * half] = (g * slope).astype(BF16)

    def forward(h, at):
        v = summed(0, h, at)
        out_send[0, at, h * half : (h + 1) * half] = (
            0.5 * v * (1.0 + lax.erf(v * 0.7071067811865476))).astype(BF16)

    rows, broad = sums.shape[1], sums.shape[2]
    step_n = broad // 4
    order = []
    low, high = 0, chips - 1
    while low <= high:
        order.append(high)
        if low < high:
            order.append(low)
        low, high = low + 1, high - 1

    def to_sib(j, z):
        return send(part.at[j, z, 1 - core], from_sib.at[j, z], sib_s.at[j, z], sib_r.at[j, z], sib)

    def to_right(j, z):
        return send(part.at[j, z, core], from_left.at[j, z], right_s.at[j, z], left_r.at[j, z], line(1))

    def to_left(j, z):
        return send(part.at[j, z, core], from_right.at[j, z], left_s.at[j, z], right_r.at[j, z], line(-1))

    def product(j, z):
        @pl.loop(0, broad // step_n)
        def _(t):
            at = pl.ds(pl.multiple_of(t * step_n, step_n), step_n)
            left = acts[2 * j, pl.ds(z * 2 * rows, 2 * rows), :]
            if j == 0:
                piece = jnp.dot(left, w_down[:, at], preferred_element_type=F32)
            else:
                piece = lax.dot_general(left, w_up[at, :], (((1,), (1,)), ((), ())),
                                        preferred_element_type=F32)
            part[j, z, 0, :, at] = piece[:rows]
            part[j, z, 1, :, at] = piece[rows:]
        to_sib(j, z).start()

    def onward(j, z):
        to_sib(j, z).wait_recv()
        part[j, z, core] = part[j, z, core] + from_sib[j, z]

        @pl.when(z > chip)
        def _():
            @pl.when(chip > 0)
            def _():
                to_right(j, z).wait_recv()
                part[j, z, core] = part[j, z, core] + from_left[j, z]

            to_right(j, z).start()

        @pl.when(z < chip)
        def _():
            @pl.when(chip < chips - 1)
            def _():
                to_left(j, z).wait_recv()
                part[j, z, core] = part[j, z, core] + from_right[j, z]

            to_left(j, z).start()


    def complete(k):
        for which in (0, 1):
            ref = acts.at[k, pl.ds(diag * tokens, tokens), pl.ds(which * half, half)]
            arrived(ref, g_r.at[k, 2 + which], (peer_y, peer_x)[which])

    gathered(2)
    load_down.wait()
    products(2)
    gathered(1)
    load_up.wait()
    products(1)
    transit(2)
    gathered(0)
    products(0)
    transit(1)
    landed(2)
    landed(1)
    transit(0)
    over(backward)
    publish(2)
    landed(0)
    over(forward)
    publish(0)
    for k in (2, 0, 1):
        acts[k, pl.ds(col * tokens, tokens), :] = out_send[k]
    pass_on(2)
    publish(1)
    complete(2)
    for z in order:
        product(1, z)
    pass_on(0)
    complete(0)
    for z in order:
        onward(1, z)
        product(0, z)
    pass_on(1)
    for z in order:
        onward(0, z)
    complete(1)
    for j in (2, 1, 0):
        finish(mine[j])
        relays(j, lambda owner, sign, copies: finish(copies))
        for which in (0, 1):
            relay(j, which).wait_send()
            first(j, which).wait_send()
        for s in range(6):
            hop(j, s).wait_send()
    for j in (0, 1):
        sums[j] = part[j, chip, core]

        @pl.when(chip > 0)
        def _():
            to_right(j, chip).wait_recv()
            sums[j] = sums[j] + from_left[j, chip]

        @pl.when(chip < chips - 1)
        def _():
            to_left(j, chip).wait_recv()
            sums[j] = sums[j] + from_right[j, chip]

    for j in (0, 1):
        for z in range(chips):
            to_sib(j, z).wait_send()
            pl.when(z > chip)(to_right(j, z).wait_send)
            pl.when(z < chip)(to_left(j, z).wait_send)


def layer(R, C, width, x_fwd, x_bwd, grad_out, gain, w_up, w_down):
    rows, columns = x_fwd.shape
    wide = w_up.shape[1]
    chips, slots = R // 2, 2 * (R // 2) - 1
    count = rows * R
    tokens, half = count // C, wide // 2
    line_block = (2, chips, rows, columns)
    return pl.pallas_call(
        functools.partial(layer_kernel, R, C, width),
        out_shape=(jax.ShapeDtypeStruct((3, count, columns), BF16),
                   jax.ShapeDtypeStruct((rows, 128), F32),
                   jax.ShapeDtypeStruct((3, count, wide), BF16),
                   jax.ShapeDtypeStruct((2, rows, columns), F32)),
        in_specs=[VMEM] * 4 + [pl.BlockSpec(memory_space=pl.ANY)] * 2,
        out_specs=(VMEM,) * 4,
        scratch_shapes=[
            pltpu.VMEM(w_up.shape, BF16), pltpu.VMEM(w_down.shape, BF16),
            pltpu.VMEM((rows, 128), F32), pltpu.VMEM((C - 1, rows, 128), F32),
            pltpu.VMEM((3, tokens, wide), BF16),
            pltpu.VMEM((3, 6, tokens, half), F32), pltpu.VMEM((3, 6, tokens, half), F32),
            pltpu.VMEM((3, 2, tokens, half), F32),
            pltpu.VMEM((2, chips, 2, rows, columns), F32),
        ]
        + [pltpu.VMEM(line_block, F32)] * 3
        + [DMA((2,)), DMA((C - 1,)), DMA((C - 1,)),
           DMA((3, slots)), DMA((3, slots)), DMA((3, slots)), DMA((3, R)),
           DMA((3, 6)), DMA((3, 6)), DMA((3, 4)), DMA((3, 4))]
        + [DMA((2, chips))] * 6,
        compiler_params=pltpu.CompilerParams(
            collective_id=0, has_side_effects=True, vmem_limit_bytes=GRANT),
        cost_estimate=pl.CostEstimate(flops=10**10, bytes_accessed=10**7, transcendentals=0),
    )(x_fwd, x_bwd, grad_out, gain, w_up, w_down)


def final_kernel(R, C, width, gn, xb, go, gain, stats, squares, dx, g_gain, total,
                 st_own, st_in, gp_own, gp_in, tt_own, tt_in,
                 st_s, st_r, gp_s, gp_r, tt_s, tt_r):
    row, col = lax.axis_index("row"), lax.axis_index("col")
    cols = [{"row": row, "col": (col + i) % C} for i in range(1, C)]
    rows = [{"row": (row + i) % R, "col": col} for i in range(1, R)]
    greet(cols + rows)
    hat, inv = normal_of(xb[...].astype(F32), stats[...], 2, width)
    grad = gn[...]
    scaled = grad * gain[...]
    st_own[...] = lanes_of([jnp.sum(scaled, 1, keepdims=True), jnp.sum(scaled * hat, 1, keepdims=True)])
    first = [send(st_own, st_in.at[i], st_s.at[i], st_r.at[i], p) for i, p in enumerate(cols)]
    for copy in first:
        copy.start()
    wide = grad.shape[1]
    gp_own[:, :wide] = jnp.broadcast_to(jnp.sum(grad * hat, 0, keepdims=True), (8, wide))
    gp_own[:, wide:] = squares[...]
    gp_in[row] = gp_own[...]
    second = [send(gp_own, gp_in.at[row], gp_s.at[i], gp_r.at[i], p) for i, p in enumerate(rows)]
    for copy in second:
        copy.start()
    for copy in second:
        copy.wait()
    gains = gp_in[0]
    for i in range(1, R):
        gains = gains + gp_in[i]
    gained = gains[:, :wide]
    g_gain[...] = gained
    tt_own[...] = gains[:, wide:] + jnp.sum(gained * gained, 1, keepdims=True)
    tt_in[col] = tt_own[...]
    third = [send(tt_own, tt_in.at[col], tt_s.at[i], tt_r.at[i], p) for i, p in enumerate(cols)]
    for copy in third:
        copy.start()
    for copy in first:
        copy.wait()
    sums = st_own[...]
    for i in range(C - 1):
        sums = sums + st_in[i]
    c1, c2 = sums[:, 0:1] / width, sums[:, 1:2] / width
    dx[...] = (go[...].astype(F32) + inv * (scaled - c1 - hat * c2)).astype(BF16)
    for copy in third:
        copy.wait()
    whole = tt_in[0]
    for i in range(1, C):
        whole = whole + tt_in[i]
    total[...] = whole


def final(R, C, width, gn, x_bwd, grad_out, gain, stats, squares):
    rows, wide = gn.shape
    return pl.pallas_call(
        functools.partial(final_kernel, R, C, width),
        out_shape=(jax.ShapeDtypeStruct((rows, wide), BF16),
                   jax.ShapeDtypeStruct((8, wide), F32),
                   jax.ShapeDtypeStruct((8, 128), F32)),
        in_specs=[VMEM] * 6,
        out_specs=(VMEM, VMEM, VMEM),
        scratch_shapes=[
            pltpu.VMEM((rows, 128), F32), pltpu.VMEM((C - 1, rows, 128), F32),
            pltpu.VMEM((8, wide + 128), F32), pltpu.VMEM((R, 8, wide + 128), F32),
            pltpu.VMEM((8, 128), F32), pltpu.VMEM((C, 8, 128), F32),
            DMA((C - 1,)), DMA((C - 1,)), DMA((R - 1,)), DMA((R - 1,)), DMA((C - 1,)), DMA((C - 1,)),
        ],
        compiler_params=pltpu.CompilerParams(
            collective_id=3, has_side_effects=True, vmem_limit_bytes=GRANT),
        cost_estimate=pl.CostEstimate(flops=10**9, bytes_accessed=10**7, transcendentals=0),
    )(gn, x_bwd, grad_out, gain, stats, squares)


def with_kernels(R, C):
    def step(x_fwd, x_bwd, grad_out, gain, w_up, w_down):
        rows, columns = x_fwd.shape
        width = columns * C
        gain_row = gain.reshape(1, columns)
        full, stats, acts, sums = layer(R, C, width, x_fwd, x_bwd, grad_out, gain_row, w_up, w_down)
        y_fwd = (x_fwd.astype(F32) + sums[0]).astype(BF16)
        down_total = contract(acts[1], full[2], 0, 0)
        up_total = contract(full[1], acts[2], 0, 0)
        squares = jnp.sum(up_total * up_total) + jnp.sum(down_total * down_total)
        dx, g_gain, total = final(R, C, width, sums[1], x_bwd, grad_out, gain_row, stats,
                                  jnp.broadcast_to(squares, (8, 128)))
        param_count = 2 * width * w_up.shape[1] * R + width
        norm_value = jnp.sqrt(total[0, 0])
        grad_rms = norm_value / math.sqrt(param_count)
        factor = jnp.minimum(1.0, clip_share * math.sqrt(param_count) / norm_value)
        return (y_fwd, dx, up_total * factor, down_total * factor, g_gain[0] * factor, grad_rms)

    return step


def solution(mesh):
    placed = (
        P("row", "col"),
        P("row", "col"),
        P("row", "col"),
        P("col"),
        P("col", "row"),
        P("row", "col"),
    )
    R, C = mesh.shape["row"], mesh.shape["col"]
    body = with_kernels(R, C) if C == 4 and R % 2 == 0 else on_device
    return jax.shard_map(
        body,
        mesh=mesh,
        in_specs=placed,
        out_specs=(
            P("row", "col"),
            P("row", "col"),
            P("col", "row"),
            P("row", "col"),
            P("col"),
            P(),
        ),
        check_vma=False,
    )
```
